32 devices in a mesh: dp: 4 (over x, core), seq: 4 (over z), tensor: 2 (over y).
Axes of the slice: x: 2, y: 2, z: 4, core: 2. Of those that a mesh axis runs over, the one named last changes fastest.
Arguments:
- query_vectors: bfloat16 [896, 4096], P(('dp', 'seq'), 'tensor'), may hold values from -128 to 128
- key_vectors: bfloat16 [896, 2048], P(('dp', 'seq'), 'tensor'), may hold values from -6 to 6
- value_vectors: bfloat16 [896, 2048], P(('dp', 'seq'), 'tensor'), may hold values from -6 to 6
- out_weight: bfloat16 [4096, 3584], P(None, 'tensor'), may hold values from -0.09375 to 0.09375
- residual: bfloat16 [896, 3584], P(('dp', 'seq'), 'tensor'), may hold values from -64 to 64
- post_gain: float32 [3584], P('tensor'), may hold values from 0.1 to 1.9
- final_gain: float32 [3584], P('tensor'), may hold values from 0.1 to 1.9
- vocab_weight: bfloat16 [16000, 3584], P(('dp', 'seq', 'tensor')), may hold values from -4 to 4
- segment_ids: int32 [4, 224], P('dp', 'seq'), may hold values from 0 to 7, as said below
- doc_starts: int32 [4, 8], P('dp'), may hold values from 0 to 223, as said below
- doc_index: int32 [4, 8], P('dp'), may hold values from 0 to 31
- targets: int32 [4, 224], replicated, may hold values from 0 to 15999
Outputs:
- token_logprob: float32 [4, 224], P('dp', 'seq')
- doc_loglik: float32 [32], replicated
- doc_counts: float32 [32], replicated
The draws below stay inside these ranges and needn't reach their ends.
Inputs may be any that keep to these rules, and one draw needn't show every extreme that they name: `segment_ids`: within each row the numbers never fall and every number 0 to 7 appears; segment s of a row begins at doc_starts[row, s]; each segment holds 1 to 168 positions. doc_starts[row, 0] = 0 and the starts rise strictly along each row.
All inputs are finite; a program needn't handle non-finite values.
Results may differ from the reference program's by a relative error of at most 0.00074.
Values may be sent and summed in bfloat16 or wider, within the bound.
A program may use at most 64 MiB of HBM per device.

```python
import math
import jax
import jax.numpy as jnp
import numpy as np
from jax import lax

D = 3584
HEADS = 16
KV_HEADS = 8
HEAD_DIM = 256
SEGS = 8
VOCAB = 16000
LENGTH = 224
ROWS = 4
TOKENS = 896
MOSTDOC = 168
NDOCS = 32


def one_row(key):
    first_key, second_key = jax.random.split(key)
    leftover = LENGTH - MOSTDOC
    picks = jax.random.permutation(first_key, leftover - 1)[:SEGS - 2] + 1
    edges = jnp.concatenate([jnp.zeros((1,), jnp.int32), jnp.sort(picks).astype(jnp.int32), jnp.full((1,), leftover, jnp.int32)])
    others = edges[1:] - edges[:-1]
    padded = jnp.concatenate([others, jnp.zeros((1,), jnp.int32)])
    place = jax.random.randint(second_key, (), 0, SEGS)
    slots = jnp.arange(SEGS, dtype=jnp.int32)
    before = padded[slots]
    after = padded[jnp.maximum(slots - 1, 0)]
    return jnp.where(slots < place, before, jnp.where(slots == place, MOSTDOC, after)).astype(jnp.int32)


def document_layout(key):
    row_keys = jax.random.split(jax.random.fold_in(key, 17), ROWS)
    lengths = jax.vmap(one_row)(row_keys)
    starts = jnp.cumsum(lengths, axis=1) - lengths
    positions = jnp.arange(LENGTH, dtype=jnp.int32)
    segment_ids = jnp.sum((positions[None, :, None] >= starts[:, None, :]).astype(jnp.int32), axis=2) - 1
    return (segment_ids.astype(jnp.int32), starts.astype(jnp.int32))


def draw_segment_ids(key, part):
    return document_layout(key)[0]


def draw_doc_starts(key, part):
    return document_layout(key)[1]


def attention_inputs(key):
    base_key, noise_key, pick_key, strength_key, gap_key = jax.random.split(jax.random.fold_in(key, 41), 5)
    keys = jnp.clip(jax.random.normal(base_key, (TOKENS, KV_HEADS, HEAD_DIM)), -6.0, 6.0)
    noise = jnp.clip(jax.random.normal(noise_key, (TOKENS, HEADS, HEAD_DIM)), -6.0, 6.0)
    picked = (jax.random.randint(pick_key, (TOKENS, HEADS), 0, 8) == 0).astype(jnp.float32)
    strength = jnp.exp(jax.random.uniform(strength_key, (TOKENS, HEADS), minval=math.log(70.0 / 16.0), maxval=math.log(150.0 / 16.0)))
    gap = jax.random.uniform(gap_key, (TOKENS, HEADS), minval=15.0 / 16.0, maxval=40.0 / 16.0)
    group_size = HEADS // KV_HEADS
    own = jnp.repeat(keys, group_size, axis=1)
    prior = jnp.repeat(jnp.roll(keys, 1, axis=0), group_size, axis=1)
    lift = picked * strength
    second = picked * (strength - gap)
    queries = noise + lift[..., None] * own + second[..., None] * prior
    queries = jnp.clip(queries, -128.0, 128.0)
    return (queries.reshape(TOKENS, HEADS * HEAD_DIM), keys.reshape(TOKENS, KV_HEADS * HEAD_DIM))


def draw_query_vectors(key, part):
    return attention_inputs(key)[0].astype(jnp.bfloat16)


def draw_key_vectors(key, part):
    return attention_inputs(key)[1].astype(jnp.bfloat16)


def residual_keys(key):
    return jax.random.split(jax.random.fold_in(key, 29), 4)


def draw_residual(key, part):
    row_key, column_key, base_key, common_key = residual_keys(key)
    row_scale = jnp.exp(jax.random.uniform(row_key, (TOKENS, 1), minval=jnp.log(0.25), maxval=jnp.log(2.5)))
    column_scale = jnp.exp(jax.random.uniform(column_key, (1, D), minval=jnp.log(0.25), maxval=jnp.log(2.5)))
    base = jnp.clip(jax.random.normal(base_key, (TOKENS, D)), -6.0, 6.0)
    return (base * row_scale * column_scale).astype(jnp.bfloat16)


def draw_vocab_weight(key, part):
    base_key = jax.random.fold_in(jax.random.fold_in(key, 53), 0)
    spread = float(D // 9) ** (-0.5)
    weights = jnp.clip(jax.random.normal(base_key, (VOCAB, D)), -6.0, 6.0) * spread
    return weights.astype(jnp.bfloat16)


def with_ends(drawn, key, smallest, high):
    dims = drawn.shape
    spot = [jax.random.randint(jax.random.fold_in(key, axis), (), 0, dims[axis]) for axis in range(len(dims))]
    drawn = drawn.at[tuple(spot)].set(smallest)
    longest = dims.index(max(dims))
    spot[longest] = (spot[longest] + 1) % dims[longest]
    return drawn.at[tuple(spot)].set(high)


def steps_of(key, extent, pieces, smallest, top_value):
    loudness, own = 1.0, jax.random.fold_in(key, 6)
    for dim, blocks in pieces:
        heights = jnp.exp(jax.random.uniform(jax.random.fold_in(own, dim), (blocks,), jnp.float32, smallest / len(pieces), top_value / len(pieces)))
        loudness = loudness * jnp.repeat(heights, extent[dim] // blocks).reshape([-1 if axis == dim else 1 for axis in range(len(extent))])
    return loudness


def rank_bounds(number_of, skew):
    loads = [(1 << 20) // math.isqrt(standing ** skew) + 1 for standing in range(1, number_of + 1)]
    scale = 1 + sum(loads) // (1 << 30)
    return np.cumsum(np.array([max(1, weight // scale) for weight in loads]))


def ranked_ids(stream_key, shape, amount, lean):
    listing = rank_bounds(amount, lean)
    pick = jax.random.randint(jax.random.fold_in(stream_key, 1), shape, 0, int(listing[amount - 1]))
    rank = jnp.searchsorted(jnp.asarray(listing, jnp.int32), pick, side="right")
    return jax.random.permutation(jax.random.fold_in(stream_key, 2), amount)[rank].astype(jnp.int32)


def gaussian(rng, shape, scale, bound, pieces=(), kind=jnp.bfloat16):
    result = jax.random.normal(rng, shape, jnp.float32) * scale
    if len(pieces) > 0:
        result = steps_of(rng, shape, pieces, -0.22, 0.18) * result
    return jnp.clip(result, min=-bound, max=bound).astype(kind)


def setup_inputs(seed: int = 0) -> dict:
    streams_of = jax.random.split(jax.random.key(seed), 13)
    return {
        "query_vectors": draw_query_vectors(jax.random.fold_in(streams_of[12], 71), 0),
        "key_vectors": draw_key_vectors(jax.random.fold_in(streams_of[12], 71), 0),
        "value_vectors": gaussian(streams_of[2], (TOKENS, KV_HEADS * HEAD_DIM), 1.0, 6.0, ((0, 16), (1, 2))),
        "out_weight": gaussian(streams_of[3], (HEADS * HEAD_DIM, D), (HEADS * HEAD_DIM) ** -0.5, 0.09375, ((1, 2),)),
        "residual": draw_residual(jax.random.fold_in(streams_of[12], 71), 0),
        "post_gain": jnp.clip(1.0 + 0.18 * jax.random.normal(streams_of[5], (D,), jnp.float32), 0.1, 1.9),
        "final_gain": jnp.clip(1.0 + 0.18 * jax.random.normal(streams_of[6], (D,), jnp.float32), 0.1, 1.9),
        "vocab_weight": draw_vocab_weight(jax.random.fold_in(streams_of[12], 71), 0),
        "segment_ids": draw_segment_ids(jax.random.fold_in(streams_of[12], 71), 0),
        "doc_starts": draw_doc_starts(jax.random.fold_in(streams_of[12], 71), 0),
        "doc_index": with_ends(jax.random.randint(streams_of[10], (ROWS, SEGS), 0, NDOCS), jax.random.fold_in(streams_of[10], 1), 0, NDOCS - 1).astype(jnp.int32),
        "targets": with_ends(ranked_ids(streams_of[11], (ROWS, LENGTH), VOCAB, 2), jax.random.fold_in(streams_of[11], 3), 0, VOCAB - 1).astype(jnp.int32),
    }


ATTENTION_CAP = 50.0
LOGIT_CAP = 30.0
EPSILON = 1e-06

def first_positions(segment_row, start_row):
    segment_match = segment_row[:, None] == jnp.arange(SEGS, dtype=jnp.int32)[None, :]
    return lax.optimization_barrier(jnp.sum(jnp.where(segment_match, start_row[None, :], 0), axis=1)).astype(jnp.int32)

def attend_row(inputs):
    query_row, key_row, value_row, segment_row, start_row = inputs
    group_size = HEADS // KV_HEADS
    query_heads = query_row.astype(jnp.float32).reshape(LENGTH, KV_HEADS, group_size, HEAD_DIM)
    key_heads = key_row.astype(jnp.float32).reshape(LENGTH, KV_HEADS, HEAD_DIM)
    value_heads = value_row.astype(jnp.float32).reshape(LENGTH, KV_HEADS, HEAD_DIM)
    raw_scores = jnp.einsum('ikgd,jkd->ikgj', query_heads, key_heads)
    capped = ATTENTION_CAP * jnp.tanh(raw_scores * HEAD_DIM ** (-0.5) / ATTENTION_CAP)
    positions = jnp.arange(LENGTH, dtype=jnp.int32)
    doc_first = first_positions(segment_row, start_row)
    visible = (positions[None, :] <= positions[:, None]) & (positions[None, :] >= doc_first[:, None])
    weights = jnp.where(visible[:, None, None, :], jnp.exp(capped), 0.0)
    denominator = lax.optimization_barrier(jnp.sum(weights, axis=-1))
    rounded = lax.optimization_barrier(weights.astype(jnp.bfloat16)).astype(jnp.float32)
    numerator = jnp.einsum('ikgj,jkd->ikgd', rounded, value_heads)
    attended = numerator / denominator[..., None]
    return attended.reshape(LENGTH, HEADS * HEAD_DIM).astype(jnp.bfloat16)

def reference(query_vectors, key_vectors, value_vectors, out_weight, residual, post_gain, final_gain, vocab_weight, segment_ids, doc_starts, doc_index, targets):
    attended = lax.map(attend_row, (query_vectors.reshape(ROWS, LENGTH, HEADS * HEAD_DIM), key_vectors.reshape(ROWS, LENGTH, KV_HEADS * HEAD_DIM), value_vectors.reshape(ROWS, LENGTH, KV_HEADS * HEAD_DIM), segment_ids, doc_starts))
    attended = attended.reshape(TOKENS, HEADS * HEAD_DIM)
    branch = jnp.dot(attended, out_weight, preferred_element_type=jnp.float32)
    branch_rms = jnp.sqrt(lax.optimization_barrier(jnp.mean(branch * branch, axis=1, keepdims=True)) + EPSILON)
    updated = residual.astype(jnp.float32) + post_gain[None, :] * branch / branch_rms
    updated_rms = jnp.sqrt(lax.optimization_barrier(jnp.mean(updated * updated, axis=1, keepdims=True)) + EPSILON)
    hidden = (final_gain[None, :] * updated / updated_rms).astype(jnp.bfloat16)
    block_rows = math.gcd(TOKENS, 256)

    def head_block(inputs):
        rows_in, label_rows = inputs
        logits = lax.dot_general(rows_in, vocab_weight, (((1,), (1,)), ((), ())), preferred_element_type=jnp.float32)
        capped = LOGIT_CAP * jnp.tanh(logits / LOGIT_CAP)
        totals = lax.optimization_barrier(jnp.sum(jnp.exp(capped), axis=1))
        chosen = jnp.take_along_axis(capped, label_rows[:, None], axis=1)[:, 0]
        return (totals, chosen)
    totals, chosen = lax.map(head_block, (hidden.reshape(TOKENS // block_rows, block_rows, D), targets.reshape(TOKENS // block_rows, block_rows)))
    totals = totals.reshape(ROWS, LENGTH)
    chosen = chosen.reshape(ROWS, LENGTH)
    positions = jnp.arange(LENGTH, dtype=jnp.int32)
    segment_slots = jnp.arange(SEGS, dtype=jnp.int32)
    next_segment = segment_ids + 1
    doc_end = lax.optimization_barrier(jnp.sum(jnp.where(segment_slots[None, None, :] == next_segment[:, :, None], doc_starts[:, None, :], 0), axis=2))
    doc_end = doc_end + jnp.where(next_segment == SEGS, LENGTH, 0)
    counted = (positions[None, :] + 1 < doc_end).astype(jnp.float32)
    token_logprob = counted * (chosen - jnp.log(totals))
    doc_of = lax.optimization_barrier(jnp.sum(jnp.where(segment_slots[None, None, :] == segment_ids[:, :, None], doc_index[:, None, :], 0), axis=2))
    doc_match = (doc_of.reshape(TOKENS)[:, None] == jnp.arange(NDOCS, dtype=jnp.int32)[None, :]).astype(jnp.float32)
    doc_loglik = lax.optimization_barrier(jnp.sum(token_logprob.reshape(TOKENS)[:, None] * doc_match, axis=0))
    doc_counts = lax.optimization_barrier(jnp.sum(counted.reshape(TOKENS)[:, None] * doc_match, axis=0))
    return (token_logprob, doc_loglik, doc_counts)
```

```python
import functools

import jax
import jax.numpy as jnp
from jax import lax
from jax.experimental import pallas as pl
from jax.experimental.pallas import tpu as pltpu
from jax.sharding import PartitionSpec as P

HEAD_DIM = 256
ATTENTION_CAP = 50.0
LOGIT_CAP = 30.0
EPSILON = 1e-06
MESH = pl.DeviceIdType.MESH
PAD = 64
NT = (((1,), (1,)), ((), ()))
NN = (((1,), (0,)), ((), ()))


def dot(a, b, dims):
    return lax.dot_general(a, b, dims, preferred_element_type=jnp.float32)


def body(
    sizes,
    q_ref, k_ref, v_ref, w_hbm, res_ref, pg_ref, fg_ref, voc_hbm, first_ref, lab_ref, meta_ref,
    lp_ref, docs_ref,
    w_ref, voc_ref, kv, num, den, att, branch, stat, hid, part, gat_dp, gat_t, gat_s,
    local_sem, kv_send, kv_recv, att_send, att_recv, st_send, st_recv,
    hid_recv, z_send, y_send, x_send, c_send,
    fd_send, fd_recv, ft_send, ft_recv, fs_send, fs_recv,
):
    ND, NZ, NY, docs = sizes
    NC = 2 if ND % 2 == 0 else 1
    NX = ND // NC
    D = voc_hbm.shape[-1] if voc_hbm.ndim == 2 else voc_hbm.shape[0] * voc_hbm.shape[2]
    me_d, me_z, me_t = lax.axis_index("dp"), lax.axis_index("seq"), lax.axis_index("tensor")
    me_x, me_c = me_d // NC, me_d % NC
    rows = q_ref.shape[0]
    kvw = k_ref.shape[1]
    groups = kvw // HEAD_DIM
    per = q_ref.shape[1] // kvw
    heads = groups * per
    qw = q_ref.shape[1]
    fw = w_hbm.shape[1]

    w_copy = pltpu.make_async_copy(w_hbm, w_ref, local_sem.at[0])
    voc_copy = pltpu.make_async_copy(voc_hbm, voc_ref, local_sem.at[1])
    w_copy.start()
    voc_copy.start()

    def dev(d=None, z=None, t=None):
        return (me_d if d is None else d, me_z if z is None else z, me_t if t is None else t)

    def remote(src, dst, send, recv, device):
        return pltpu.make_async_remote_copy(
            src_ref=src, dst_ref=dst, send_sem=send, recv_sem=recv, device_id=device, device_id_type=MESH
        )

    def others(me, n):
        return [lax.rem(me + i, n) for i in range(1, n)]

    barrier = pltpu.get_barrier_semaphore()
    peers = [dev(d=p) for p in others(me_d, ND)]
    peers += [dev(z=p) for p in others(me_z, NZ)]
    peers += [dev(t=p) for p in others(me_t, NY)]
    for p in peers:
        pl.semaphore_signal(barrier, inc=1, device_id=p, device_id_type=MESH)
    pl.semaphore_wait(barrier, len(peers))

    def kv_copy(s, which):
        src = (k_ref, v_ref)[which] if s == 0 else kv.at[s, which]
        return remote(
            src, kv.at[s + 1, which], kv_send.at[s, which], kv_recv.at[s + 1, which],
            dev(z=lax.rem(me_z + 1, NZ)),
        )

    i_pos = lax.broadcasted_iota(jnp.int32, (rows, rows), 0)
    j_pos = lax.broadcasted_iota(jnp.int32, (rows, rows), 1)
    first = first_ref[...]
    for s in range(NZ):
        @pl.when(me_z >= s)
        def _(s=s):
            for which in range(2):
                if s > 0:
                    remote(
                        kv.at[s, which], kv.at[s, which], kv_send.at[s - 1, which], kv_recv.at[s, which], dev()
                    ).wait_recv()
                if s < NZ - 1:
                    @pl.when(me_z + 1 < NZ)
                    def _():
                        kv_copy(s, which).start()
            key_pos = (me_z - s) * rows + j_pos
            seen = key_pos >= first
            if s == 0:
                seen = seen & (j_pos <= i_pos)
            for h in range(heads):
                cols = slice(h // per * HEAD_DIM, (h // per + 1) * HEAD_DIM)
                kk = k_ref[:, cols] if s == 0 else kv[s, 0, :, cols]
                vv = v_ref[:, cols] if s == 0 else kv[s, 1, :, cols]
                raw = dot(q_ref[:, h * HEAD_DIM:(h + 1) * HEAD_DIM], kk, NT)
                capped = ATTENTION_CAP * jnp.tanh(raw * (HEAD_DIM ** (-0.5) / ATTENTION_CAP))
                wt = jnp.where(seen, jnp.exp(capped), 0.0)
                top = dot(wt.astype(jnp.bfloat16), vv, NN)
                low = jnp.broadcast_to(jnp.sum(wt, axis=1, keepdims=True), (rows, 128))
                if s == 0:
                    num[h] = top
                    den[h] = low
                else:
                    num[h] = num[h] + top
                    den[h] = den[h] + low

    def att_copy(part_id, peer, idx):
        width = qw // 2
        ref = att.at[me_t, :, pl.ds(part_id * width, width)]
        return remote(ref, ref, att_send.at[idx, part_id], att_recv.at[me_t, part_id], dev(t=peer))

    for half in range(2):
        for h in range(half * heads // 2, (half + 1) * heads // 2):
            att[me_t, :, h * HEAD_DIM:(h + 1) * HEAD_DIM] = (num[h] / den[h][:, :1]).astype(jnp.bfloat16)
        for i, p in enumerate(others(me_t, NY)):
            att_copy(half, p, i).start()

    w_copy.wait()
    step = 256 if fw % 256 == 0 else fw

    def project(t, begin):
        base = pl.multiple_of(t * qw, qw)
        for n in range(fw // step):
            got = dot(att[t], w_ref[pl.ds(base, qw), n * step:(n + 1) * step], NN)
            cols = slice(n * step, (n + 1) * step)
            branch[:, cols] = got if begin else branch[:, cols] + got

    project(me_t, True)
    for p in others(me_t, NY):
        for half in range(2):
            width = qw // 2
            ref = att.at[p, :, pl.ds(half * width, width)]
            remote(ref, ref, att_send.at[0, 0], att_recv.at[p, half], dev()).wait_recv()
        project(p, False)

    br = branch[...]
    carried = res_ref[...].astype(jnp.float32)
    gained = pg_ref[...] * br
    lane = lax.broadcasted_iota(jnp.int32, (rows, 128), 1)
    packed = jnp.zeros((rows, 128), jnp.float32)
    for i, prod in enumerate((br * br, carried * carried, carried * gained, gained * gained)):
        packed = jnp.where(lane == i, jnp.sum(prod, axis=1, keepdims=True), packed)
    stat[me_t] = packed

    def stat_copy(peer, i):
        return remote(stat.at[me_t], stat.at[me_t], st_send.at[i], st_recv.at[me_t], dev(t=peer))

    for i, p in enumerate(others(me_t, NY)):
        stat_copy(p, i).start()
    for p in others(me_t, NY):
        remote(stat.at[p], stat.at[p], st_send.at[0], st_recv.at[p], dev()).wait_recv()
    total = stat[0]
    for t in range(1, NY):
        total = total + stat[t]
    sq_branch, sq_carried, cross, sq_gained = (total[:, i:i + 1] for i in range(4))
    inv_branch = 1.0 / jnp.sqrt(sq_branch / D + EPSILON)
    sq_total = sq_carried + 2.0 * inv_branch * cross + inv_branch * inv_branch * sq_gained
    inv_total = 1.0 / jnp.sqrt(sq_total / D + EPSILON)
    hid[me_d, me_z, me_t, :rows, :] = (
        fg_ref[...] * (carried + gained * inv_branch) * inv_total
    ).astype(jnp.bfloat16)

    def slot(d, z, t):
        return hid.at[d, z, t, pl.ds(0, rows), :]

    def send(d, z, t, sem, device):
        return remote(slot(d, z, t), slot(d, z, t), sem, hid_recv.at[d, z, t], device)

    def landed(d, z, t):
        send(d, z, t, z_send.at[0, 0], dev()).wait_recv()

    y_peers = others(me_t, NY)
    x_peers = [p * NC + me_c for p in others(me_x, NX)]
    twin = [me_x * NC + 1 - me_c] if NC == 2 else []
    offsets = [0]
    for i in range(1, NZ):
        offsets += [-i, i]

    def y_first(z):
        return lax.rem(z + me_c, 2) == 0

    def guarded(off, fn):
        if off == 0:
            fn(me_z)
        else:
            @pl.when((me_z + off >= 0) & (me_z + off < NZ))
            def _():
                fn(me_z + off)

    def to_twin(d, z, t, act):
        for p in twin:
            act(send(d, z, t, c_send.at[d // NC, z, t], dev(d=p)))

    def column(z, off, act, wait):
        if wait and off != 0:
            landed(me_d, z, me_t)
        if off <= 0:
            @pl.when(me_z + 1 < NZ)
            def _():
                act(send(me_d, z, me_t, z_send.at[z, 0], dev(z=lax.rem(me_z + 1, NZ))))
        if off >= 0:
            @pl.when(me_z >= 1)
            def _():
                act(send(me_d, z, me_t, z_send.at[z, 1], dev(z=lax.rem(me_z + NZ - 1, NZ))))
        for i, p in enumerate(y_peers):
            act(send(me_d, z, me_t, y_send.at[0, z, i], dev(t=p)))
        for i, p in enumerate(x_peers):
            act(send(me_d, z, me_t, x_send.at[0, z, i], dev(d=p)))
        to_twin(me_d, z, me_t, act)

    def across(z, act, wait):
        for j, t in enumerate(y_peers):
            if wait:
                landed(me_d, z, t)
            if x_peers:
                @pl.when(y_first(z))
                def _(j=j, t=t):
                    for i, p in enumerate(x_peers):
                        act(send(me_d, z, t, x_send.at[1 + j, z, i], dev(d=p)))
            to_twin(me_d, z, t, act)
        for j, d in enumerate(x_peers):
            if wait:
                landed(d, z, me_t)
            if y_peers:
                @pl.when(jnp.logical_not(y_first(z)))
                def _(j=j, d=d):
                    for i, p in enumerate(y_peers):
                        act(send(d, z, me_t, y_send.at[1 + j, z, i], dev(t=p)))
            to_twin(d, z, me_t, act)

    def diagonal(z, act, wait):
        for d in x_peers:
            for t in y_peers:
                if wait:
                    landed(d, z, t)
                to_twin(d, z, t, act)

    def start(c):
        c.start()

    guarded(offsets[0], lambda z: column(z, 0, start, True))
    for n in range(1, len(offsets) + 1):
        if n < len(offsets):
            guarded(offsets[n], lambda z: column(z, offsets[n], start, True))
        guarded(offsets[n - 1], lambda z: across(z, start, True))

    voc_copy.wait()
    count = voc_ref.shape[-2]
    base = ((me_d * NZ + me_z) * NY + me_t) * count
    vocab_ids = base + lax.broadcasted_iota(jnp.int32, (count, NZ * PAD), 0)
    per_row = NZ * PAD // 128
    R = ND * per_row

    def logits_of(d):
        acc = None
        for t in range(NY):
            left = voc_ref[:, t * fw:(t + 1) * fw] if len(voc_ref.shape) == 2 else voc_ref[t]
            got = dot(left, hid[d, :, t].reshape(NZ * PAD, fw), NT)
            acc = got if acc is None else acc + got
        capped = LOGIT_CAP * jnp.tanh(acc * (1.0 / LOGIT_CAP))
        tot = jnp.sum(jnp.exp(capped), axis=0, keepdims=True)
        cho = jnp.sum(jnp.where(vocab_ids == lab_ref[d], capped, 0.0), axis=0, keepdims=True)
        for r in range(per_row):
            part[pl.ds(d * per_row + r, 1), :] = tot[:, r * 128:(r + 1) * 128]
            part[pl.ds(R + d * per_row + r, 1), :] = cho[:, r * 128:(r + 1) * 128]

    logits_of(me_d)
    for d in twin:
        for z in range(NZ):
            for t in range(NY):
                landed(d, z, t)
        logits_of(d)
    for off in offsets:
        guarded(off, lambda z: diagonal(z, start, True))
    for d in x_peers:
        logits_of(d)
    if NC == 2:
        for p in others(me_x, NX):
            d = p * NC + 1 - me_c
            for z in range(NZ):
                for t in range(NY):
                    landed(d, z, t)
            logits_of(d)
    part[2 * R:4 * R, :] = meta_ref[...]

    def exchange(buf, me, n, sends, recvs, where):
        buf[me] = part[...]

        def copy(p, i):
            return remote(buf.at[me], buf.at[me], sends.at[i], recvs.at[me], where(p))

        for i, p in enumerate(others(me, n)):
            copy(p, i).start()
        for p in others(me, n):
            remote(buf.at[p], buf.at[p], sends.at[0], recvs.at[p], dev()).wait_recv()
        out = buf[0]
        for j in range(1, n):
            out = out + buf[j]
        part[...] = out
        return lambda: [copy(p, i).wait_send() for i, p in enumerate(others(me, n))]

    drains = [
        exchange(gat_dp, me_d, ND, fd_send, fd_recv, lambda p: dev(d=p)),
        exchange(gat_t, me_t, NY, ft_send, ft_recv, lambda p: dev(t=p)),
        exchange(gat_s, me_z, NZ, fs_send, fs_recv, lambda p: dev(z=p)),
    ]
    totals, chosen = part[0:R, :], part[R:2 * R, :]
    counted, doc = part[2 * R:3 * R, :], part[3 * R:4 * R, :]
    inside = lax.rem(lax.broadcasted_iota(jnp.int32, (R, 128), 1), PAD) < rows
    counted = jnp.where(inside, counted, 0.0)
    logprob = jnp.where(inside, counted * (chosen - jnp.log(totals)), 0.0)
    lp_ref[...] = logprob
    names = lax.broadcasted_iota(jnp.int32, (docs, 128), 0).astype(jnp.float32)
    like = jnp.zeros((docs, 128), jnp.float32)
    cnt = jnp.zeros((docs, 128), jnp.float32)
    for r in range(R):
        hit = names == doc[r:r + 1, :]
        like = like + jnp.where(hit, logprob[r:r + 1, :], 0.0)
        cnt = cnt + jnp.where(hit, counted[r:r + 1, :], 0.0)
    col = lax.broadcasted_iota(jnp.int32, (docs, 128), 1)
    docs_ref[...] = jnp.where(
        col == 0, jnp.sum(like, axis=1, keepdims=True), jnp.sum(cnt, axis=1, keepdims=True)
    )

    def drain(c):
        c.wait_send()

    for s in range(NZ - 1):
        @pl.when((me_z >= s) & (me_z + 1 < NZ))
        def _(s=s):
            for which in range(2):
                kv_copy(s, which).wait_send()
    for i, p in enumerate(others(me_t, NY)):
        for half in range(2):
            att_copy(half, p, i).wait_send()
        stat_copy(p, i).wait_send()
    for off in offsets:
        guarded(off, lambda z: column(z, off, drain, False))
        guarded(off, lambda z: across(z, drain, False))
        guarded(off, lambda z: diagonal(z, drain, False))
    for d in drains:
        d()


def local(
    mesh, query_vectors, key_vectors, value_vectors, out_weight, residual, post_gain, final_gain,
    vocab_weight, segment_ids, doc_starts, doc_index, targets,
):
    ND, NZ, NY = mesh.shape["dp"], mesh.shape["seq"], mesh.shape["tensor"]
    rows = query_vectors.shape[0]
    seg_row, starts = segment_ids[0], doc_starts[0]
    seg_count = starts.shape[0]
    docs = seg_count * ND
    slots = jnp.arange(seg_count, dtype=jnp.int32)
    me_d, me_z, me_t = lax.axis_index("dp"), lax.axis_index("seq"), lax.axis_index("tensor")
    positions = me_z * rows + jnp.arange(rows, dtype=jnp.int32)
    match = seg_row[:, None] == slots[None, :]
    doc_first = jnp.sum(jnp.where(match, starts[None, :], 0), axis=1, keepdims=True)
    ends = jnp.concatenate([starts[1:], jnp.full((1,), rows * NZ, jnp.int32)])
    doc_end = jnp.sum(jnp.where(match, ends[None, :], 0), axis=1)
    counted = (positions + 1 < doc_end).astype(jnp.float32)
    doc_of = jnp.sum(jnp.where(match, doc_index[0][None, :], 0), axis=1).astype(jnp.float32)
    blocks = ND * NZ
    mine = (jnp.arange(blocks)[None, :, None] == me_d * NZ + me_z) & (me_t == 0)
    facts = jnp.pad(jnp.stack([counted, doc_of]), ((0, 0), (0, PAD - rows)))
    meta = jnp.where(mine, facts[:, None, :], 0.0).reshape(2 * blocks * PAD // 128, 128)
    labels = jnp.pad(targets.reshape(ND, NZ, rows), ((0, 0), (0, 0), (0, PAD - rows))).reshape(ND, 1, NZ * PAD)
    fw = out_weight.shape[1]
    voc = vocab_weight
    if fw % 128 != 0:
        voc = voc.reshape(voc.shape[0], NY, fw).transpose(1, 0, 2)
    kvw, qw = key_vectors.shape[1], query_vectors.shape[1]
    heads = qw // HEAD_DIM
    NC = 2 if ND % 2 == 0 else 1
    NX = ND // NC
    R = blocks * PAD // 128
    f32, bf16 = jnp.float32, jnp.bfloat16
    dma = pltpu.SemaphoreType.DMA
    vm = pl.BlockSpec(memory_space=pltpu.VMEM)
    anyspace = pl.BlockSpec(memory_space=pl.ANY)
    logprob, sums = pl.pallas_call(
        functools.partial(body, (ND, NZ, NY, docs)),
        out_shape=(jax.ShapeDtypeStruct((R, 128), f32), jax.ShapeDtypeStruct((docs, 128), f32)),
        in_specs=[vm, vm, vm, anyspace, vm, vm, vm, anyspace, vm, vm, vm],
        out_specs=(vm, vm),
        scratch_shapes=[
            pltpu.VMEM(out_weight.shape, bf16),
            pltpu.VMEM(voc.shape, bf16),
            pltpu.VMEM((NZ, 2, rows, kvw), bf16),
            pltpu.VMEM((heads, rows, HEAD_DIM), f32),
            pltpu.VMEM((heads, rows, 128), f32),
            pltpu.VMEM((NY, rows, qw), bf16),
            pltpu.VMEM((rows, fw), f32),
            pltpu.VMEM((NY, rows, 128), f32),
            pltpu.VMEM((ND, NZ, NY, PAD, fw), bf16),
            pltpu.VMEM((4 * R, 128), f32),
            pltpu.VMEM((ND, 4 * R, 128), f32),
            pltpu.VMEM((NY, 4 * R, 128), f32),
            pltpu.VMEM((NZ, 4 * R, 128), f32),
            dma((2,)),
            dma((NZ, 2)), dma((NZ, 2)),
            dma((NY, 2)), dma((NY, 2)),
            dma((NY,)), dma((NY,)),
            dma((ND, NZ, NY)),
            dma((NZ, 2)),
            dma((NX, NZ, NY)),
            dma((NY, NZ, NX)),
            dma((NX, NZ, NY)),
            dma((ND,)), dma((ND,)),
            dma((NY,)), dma((NY,)),
            dma((NZ,)), dma((NZ,)),
        ],
        compiler_params=pltpu.CompilerParams(
            collective_id=0, has_side_effects=True, vmem_limit_bytes=60 * 1024 * 1024
        ),
        name="packed_loglik",
    )(
        query_vectors, key_vectors, value_vectors, out_weight, residual, post_gain[None, :],
        final_gain[None, :], voc, doc_first, labels, meta,
    )
    mine_lp = lax.dynamic_slice_in_dim(logprob.reshape(blocks, PAD), me_d * NZ + me_z, 1, axis=0)
    return (mine_lp[:, :rows], sums[:, 0], sums[:, 1])


def solution(mesh):
    in_specs = (
        P(("dp", "seq"), "tensor"),
        P(("dp", "seq"), "tensor"),
        P(("dp", "seq"), "tensor"),
        P(None, "tensor"),
        P(("dp", "seq"), "tensor"),
        P("tensor"),
        P("tensor"),
        P(("dp", "seq", "tensor"), None),
        P("dp", "seq"),
        P("dp", None),
        P("dp", None),
        P(),
    )
    out_specs = (P("dp", "seq"), P(), P())
    return jax.shard_map(
        functools.partial(local, mesh), mesh=mesh, in_specs=in_specs, out_specs=out_specs, check_vma=False
    )
```

```python
import functools

import jax
import jax.numpy as jnp
from jax import lax
from jax.experimental import pallas as pl
from jax.experimental.pallas import tpu as pltpu
from jax.sharding import PartitionSpec as P

HEAD_DIM = 256
ATTENTION_CAP = 50.0
LOGIT_CAP = 30.0
EPSILON = 1e-06
MESH = pl.DeviceIdType.MESH
PAD = 64
NT = (((1,), (1,)), ((), ()))
NN = (((1,), (0,)), ((), ()))


def dot(a, b, dims):
    return lax.dot_general(a, b, dims, preferred_element_type=jnp.float32)


def body(
    sizes,
    q_ref, k_ref, v_ref, w_hbm, res_ref, pg_ref, fg_ref, voc_hbm, seg_ref, start_ref, index_ref, target_ref,
    lp_ref, like_ref, cnt_ref,
    w_ref, voc_ref, kv, num, den, att, branch, stat, hid, held, lab_ref, part, gat_dp, gat_t, gat_s,
    local_sem, kv_send, kv_recv, att_send, att_recv, st_send, st_recv,
    hid_recv, z_send, y_send, x_send, c_send,
    fd_send, fd_recv, ft_send, ft_recv, fs_send, fs_recv,
):
    ND, NZ, NY, docs = sizes
    NC = 2 if ND % 2 == 0 else 1
    NX = ND // NC
    D = voc_hbm.shape[-1] if voc_hbm.ndim == 2 else voc_hbm.shape[0] * voc_hbm.shape[2]
    me_d, me_z, me_t = lax.axis_index("dp"), lax.axis_index("seq"), lax.axis_index("tensor")
    me_x, me_c = me_d // NC, me_d % NC
    rows = q_ref.shape[0]
    kvw = k_ref.shape[1]
    groups = kvw // HEAD_DIM
    per = q_ref.shape[1] // kvw
    heads = groups * per
    qw = q_ref.shape[1]
    fw = w_hbm.shape[1]

    w_copy = pltpu.make_async_copy(w_hbm, w_ref, local_sem.at[0])
    voc_copy = pltpu.make_async_copy(voc_hbm, voc_ref, local_sem.at[1])
    w_copy.start()
    voc_copy.start()

    def dev(d=None, z=None, t=None):
        return (me_d if d is None else d, me_z if z is None else z, me_t if t is None else t)

    def remote(src, dst, send, recv, device):
        return pltpu.make_async_remote_copy(
            src_ref=src, dst_ref=dst, send_sem=send, recv_sem=recv, device_id=device, device_id_type=MESH
        )

    def others(me, n):
        return [lax.rem(me + i, n) for i in range(1, n)]

    barrier = pltpu.get_barrier_semaphore()
    peers = [dev(d=p) for p in others(me_d, ND)]
    peers += [dev(z=p) for p in others(me_z, NZ)]
    peers += [dev(t=p) for p in others(me_t, NY)]
    for p in peers:
        pl.semaphore_signal(barrier, inc=1, device_id=p, device_id_type=MESH)
    pl.semaphore_wait(barrier, len(peers))

    def kv_copy(block, g):
        cols = pl.ds(g * HEAD_DIM, HEAD_DIM)
        up = dev(z=lax.rem(me_z + 1, NZ))
        if block is None:
            pairs = [(k_ref.at[:, cols], kv.at[me_z, 0, :, cols]), (v_ref.at[:, cols], kv.at[me_z, 1, :, cols])]
            where = me_z
        else:
            pairs = [(kv.at[block, i, :, cols],) * 2 for i in range(2)]
            where = block
        return [
            remote(src, dst, kv_send.at[where, g, i], kv_recv.at[where, g, i], up)
            for i, (src, dst) in enumerate(pairs)
        ]

    @pl.when(me_z + 1 < NZ)
    def _():
        for g in range(groups):
            for c in kv_copy(None, g):
                c.start()

    seg = seg_ref[...]
    first_row = jnp.zeros((1, rows), jnp.int32)
    end_row = jnp.zeros((1, rows), jnp.int32)
    doc_row = jnp.zeros((1, rows), jnp.int32)
    segs = start_ref.shape[1]
    for n in range(segs):
        here = seg == n
        first_row = jnp.where(here, start_ref[0, n], first_row)
        end_row = jnp.where(here, start_ref[0, n + 1] if n + 1 < segs else rows * NZ, end_row)
        doc_row = jnp.where(here, index_ref[0, n], doc_row)
    spot = me_z * rows + lax.broadcasted_iota(jnp.int32, (1, rows), 1)
    code_row = doc_row + jnp.where(spot + 1 < end_row, docs, 0)
    i_pos = lax.broadcasted_iota(jnp.int32, (rows, rows), 0)
    j_pos = lax.broadcasted_iota(jnp.int32, (rows, rows), 1)

    def column_of(row):
        full = jnp.broadcast_to(row.astype(jnp.float32), (rows, rows))
        return jnp.sum(jnp.where(i_pos == j_pos, full, 0.0), axis=1, keepdims=True)

    first = column_of(first_row).astype(jnp.int32)
    per_line = 128 // PAD
    my_block = me_d * NZ + me_z
    lanes = lax.broadcasted_iota(jnp.int32, (rows, 128), 1)
    sub = lax.broadcasted_iota(jnp.int32, (rows, 128), 0)
    placed = jnp.where(lanes == sub + lax.rem(my_block, per_line) * PAD, column_of(code_row), 0.0)
    code_line = jnp.sum(placed, axis=0, keepdims=True) * jnp.where(me_t == 0, 1.0, 0.0)
    gap = jnp.zeros((1, PAD - rows), jnp.int32)
    for d in range(ND):
        pieces = []
        for z in range(NZ):
            pieces += [target_ref[d:d + 1, z * rows:(z + 1) * rows], gap]
        lab_ref[d] = jnp.concatenate(pieces, axis=1)

    def attend(block, g):
        cols = slice(g * HEAD_DIM, (g + 1) * HEAD_DIM)
        if block is None:
            kk, vv = k_ref[:, cols], v_ref[:, cols]
            seen = (me_z * rows + j_pos >= first) & (j_pos <= i_pos)
        else:
            kk, vv = kv[block, 0, :, cols], kv[block, 1, :, cols]
            seen = block * rows + j_pos >= first
        for h in range(g * per, (g + 1) * per):
            raw = dot(q_ref[:, h * HEAD_DIM:(h + 1) * HEAD_DIM], kk, NT)
            capped = ATTENTION_CAP * jnp.tanh(raw * (HEAD_DIM ** (-0.5) / ATTENTION_CAP))
            wt = jnp.where(seen, jnp.exp(capped), 0.0)
            top = dot(wt.astype(jnp.bfloat16), vv, NN)
            low = jnp.broadcast_to(jnp.sum(wt, axis=1, keepdims=True), (rows, 128))
            if block is None:
                num[h] = top
                den[h] = low
            else:
                num[h] = num[h] + top
                den[h] = den[h] + low

    def arrived(block, g):
        for c in kv_copy(block, g):
            c.wait_recv()

        @pl.when(me_z + 1 < NZ)
        def _():
            for c in kv_copy(block, g):
                c.start()

    for g in range(groups):
        attend(None, g)
    for block in range(NZ - 2, 0, -1):
        @pl.when(block < me_z)
        def _(block=block):
            for g in range(groups):
                arrived(block, g)
                attend(block, g)

    gw = per * HEAD_DIM

    def att_copy(g, peer, idx):
        ref = att.at[me_t, :, pl.ds(g * gw, gw)]
        return remote(ref, ref, att_send.at[idx, g], att_recv.at[me_t, g], dev(t=peer))

    step = 256 if fw % 256 == 0 else fw

    def project(t, g, begin):
        base = pl.multiple_of(t * qw + g * gw, gw)
        left = att[t, :, g * gw:(g + 1) * gw]
        for n in range(fw // step):
            cols = slice(n * step, (n + 1) * step)
            got = dot(left, w_ref[pl.ds(base, gw), cols], NN)
            branch[:, cols] = got if begin else branch[:, cols] + got

    for g in range(groups):
        if NZ > 1:
            @pl.when(me_z > 0)
            def _(g=g):
                arrived(0, g)
                attend(0, g)
        for h in range(g * per, (g + 1) * per):
            att[me_t, :, h * HEAD_DIM:(h + 1) * HEAD_DIM] = (num[h] / den[h][:, :1]).astype(jnp.bfloat16)
        for i, p in enumerate(others(me_t, NY)):
            att_copy(g, p, i).start()
        if g == 0:
            w_copy.wait()
        project(me_t, g, g == 0)
    for g in range(groups):
        for p in others(me_t, NY):
            ref = att.at[p, :, pl.ds(g * gw, gw)]
            remote(ref, ref, att_send.at[0, 0], att_recv.at[p, g], dev()).wait_recv()
            project(p, g, False)

    br = branch[...]
    carried = res_ref[...].astype(jnp.float32)
    gained = pg_ref[...].reshape(1, fw) * br
    lane = lax.broadcasted_iota(jnp.int32, (rows, 128), 1)
    packed = jnp.zeros((rows, 128), jnp.float32)
    for i, prod in enumerate((br * br, carried * carried, carried * gained, gained * gained)):
        packed = jnp.where(lane == i, jnp.sum(prod, axis=1, keepdims=True), packed)
    stat[me_t] = packed

    def stat_copy(peer, i):
        return remote(stat.at[me_t], stat.at[me_t], st_send.at[i], st_recv.at[me_t], dev(t=peer))

    for i, p in enumerate(others(me_t, NY)):
        stat_copy(p, i).start()
    for p in others(me_t, NY):
        remote(stat.at[p], stat.at[p], st_send.at[0], st_recv.at[p], dev()).wait_recv()
    total = stat[0]
    for t in range(1, NY):
        total = total + stat[t]
    sq_branch, sq_carried, cross, sq_gained = (total[:, i:i + 1] for i in range(4))
    inv_branch = 1.0 / jnp.sqrt(sq_branch / D + EPSILON)
    sq_total = sq_carried + 2.0 * inv_branch * cross + inv_branch * inv_branch * sq_gained
    inv_total = 1.0 / jnp.sqrt(sq_total / D + EPSILON)
    hid[me_d, me_z, me_t, :rows, :] = (
        fg_ref[...].reshape(1, fw) * (carried + gained * inv_branch) * inv_total
    ).astype(jnp.bfloat16)

    def slot(d, z, t):
        return hid.at[d, z, t, pl.ds(0, rows), :]

    def send(d, z, t, sem, device):
        return remote(slot(d, z, t), slot(d, z, t), sem, hid_recv.at[d, z, t], device)

    def landed(d, z, t):
        send(d, z, t, z_send.at[0, 0], dev()).wait_recv()

    y_peers = others(me_t, NY)
    x_peers = [p * NC + me_c for p in others(me_x, NX)]
    twin = [me_x * NC + 1 - me_c] if NC == 2 else []
    offsets = [0]
    for i in range(1, NZ):
        offsets += [-i, i]

    def y_first(z):
        return lax.rem(z + me_c, 2) == 0

    def guarded(off, fn):
        if off == 0:
            fn(me_z)
        else:
            @pl.when((me_z + off >= 0) & (me_z + off < NZ))
            def _():
                fn(me_z + off)

    def to_twin(d, z, t, act):
        for p in twin:
            act(send(d, z, t, c_send.at[d // NC, z, t], dev(d=p)))

    def column(z, off, act, wait):
        if wait and off != 0:
            landed(me_d, z, me_t)
        if off <= 0:
            @pl.when(me_z + 1 < NZ)
            def _():
                act(send(me_d, z, me_t, z_send.at[z, 0], dev(z=lax.rem(me_z + 1, NZ))))
        if off >= 0:
            @pl.when(me_z >= 1)
            def _():
                act(send(me_d, z, me_t, z_send.at[z, 1], dev(z=lax.rem(me_z + NZ - 1, NZ))))
        for i, p in enumerate(y_peers):
            act(send(me_d, z, me_t, y_send.at[0, z, i], dev(t=p)))
        for i, p in enumerate(x_peers):
            act(send(me_d, z, me_t, x_send.at[0, z, i], dev(d=p)))
        to_twin(me_d, z, me_t, act)

    def across(z, act, wait):
        for j, t in enumerate(y_peers):
            if wait:
                landed(me_d, z, t)
            if x_peers:
                @pl.when(y_first(z))
                def _(j=j, t=t):
                    for i, p in enumerate(x_peers):
                        act(send(me_d, z, t, x_send.at[1 + j, z, i], dev(d=p)))
            to_twin(me_d, z, t, act)
        for j, d in enumerate(x_peers):
            if wait:
                landed(d, z, me_t)
            if y_peers:
                @pl.when(jnp.logical_not(y_first(z)))
                def _(j=j, d=d):
                    for i, p in enumerate(y_peers):
                        act(send(d, z, me_t, y_send.at[1 + j, z, i], dev(t=p)))
            to_twin(d, z, me_t, act)

    def diagonal(z, act, wait):
        for d in x_peers:
            for t in y_peers:
                if wait:
                    landed(d, z, t)
                to_twin(d, z, t, act)

    def start(c):
        c.start()

    guarded(offsets[0], lambda z: column(z, 0, start, True))
    for n in range(1, len(offsets) + 1):
        if n < len(offsets):
            guarded(offsets[n], lambda z: column(z, offsets[n], start, True))
        guarded(offsets[n - 1], lambda z: across(z, start, True))

    voc_copy.wait()
    count = voc_ref.shape[-2]
    base = ((me_d * NZ + me_z) * NY + me_t) * count
    vocab_ids = base + lax.broadcasted_iota(jnp.int32, (count, NZ * PAD), 0)
    per_row = NZ * PAD // 128
    R = ND * per_row

    def product(d, t):
        if len(voc_ref.shape) == 2:
            start_col = t * fw if isinstance(t, int) else pl.multiple_of(t * fw, 128)
            left = voc_ref[:, pl.ds(start_col, fw)]
        else:
            left = voc_ref[t]
        return dot(left, hid[d, :, t].reshape(NZ * PAD, fw), NT)

    def finish(d, acc):
        capped = LOGIT_CAP * jnp.tanh(acc * (1.0 / LOGIT_CAP))
        tot = jnp.sum(jnp.exp(capped), axis=0, keepdims=True)
        cho = jnp.sum(jnp.where(vocab_ids == lab_ref[d], capped, 0.0), axis=0, keepdims=True)
        for r in range(per_row):
            part[pl.ds(d * per_row + r, 1), :] = tot[:, r * 128:(r + 1) * 128]
            part[pl.ds(R + d * per_row + r, 1), :] = cho[:, r * 128:(r + 1) * 128]

    def logits_of(d):
        acc = product(d, 0)
        for t in range(1, NY):
            acc = acc + product(d, t)
        finish(d, acc)

    part[2 * R:3 * R, :] = jnp.zeros((R, 128), jnp.float32)
    part[pl.ds(2 * R + my_block // per_line, 1), :] = code_line
    logits_of(me_d)
    for d in twin:
        for z in range(NZ):
            for t in range(NY):
                landed(d, z, t)
        logits_of(d)
    far = [p * NC + 1 - me_c for p in others(me_x, NX)] if NC == 2 else []
    for i, d in enumerate(x_peers):
        held[i] = product(d, me_t)
    for i, d in enumerate(far):
        for z in range(NZ):
            landed(d, z, me_t)
        held[NX - 1 + i] = product(d, me_t)
    for off in offsets:
        guarded(off, lambda z: diagonal(z, start, True))
    for i, d in enumerate(x_peers):
        acc = held[i]
        for t in y_peers:
            acc = acc + product(d, t)
        finish(d, acc)
    for i, d in enumerate(far):
        acc = held[NX - 1 + i]
        for t in y_peers:
            for z in range(NZ):
                landed(d, z, t)
            acc = acc + product(d, t)
        finish(d, acc)

    def exchange(buf, me, n, sends, recvs, where):
        buf[me] = part[...]

        def copy(p, i):
            return remote(buf.at[me], buf.at[me], sends.at[i], recvs.at[me], where(p))

        for i, p in enumerate(others(me, n)):
            copy(p, i).start()
        for p in others(me, n):
            remote(buf.at[p], buf.at[p], sends.at[0], recvs.at[p], dev()).wait_recv()
        out = buf[0]
        for j in range(1, n):
            out = out + buf[j]
        part[...] = out
        return lambda: [copy(p, i).wait_send() for i, p in enumerate(others(me, n))]

    drains = [
        exchange(gat_dp, me_d, ND, fd_send, fd_recv, lambda p: dev(d=p)),
        exchange(gat_t, me_t, NY, ft_send, ft_recv, lambda p: dev(t=p)),
        exchange(gat_s, me_z, NZ, fs_send, fs_recv, lambda p: dev(z=p)),
    ]
    totals, chosen = part[0:R, :], part[R:2 * R, :]
    code = part[2 * R:3 * R, :]
    inside = lax.rem(lax.broadcasted_iota(jnp.int32, (R, 128), 1), PAD) < rows
    counted = jnp.where(inside & (code >= docs), 1.0, 0.0)
    doc = jnp.where(code >= docs, code - docs, code)
    logprob = jnp.where(inside, counted * (chosen - jnp.log(totals)), 0.0)
    part[0:R, :] = logprob
    line = part[pl.ds(my_block // per_line, 1), :]
    mine = line[:, :rows]
    for k in range(1, per_line):
        mine = jnp.where(lax.rem(my_block, per_line) == k, line[:, k * PAD:k * PAD + rows], mine)
    lp_ref[...] = mine
    names = lax.broadcasted_iota(jnp.int32, (docs, 128), 0).astype(jnp.float32)
    like = jnp.zeros((docs, 128), jnp.float32)
    cnt = jnp.zeros((docs, 128), jnp.float32)
    for r in range(R):
        hit = names == doc[r:r + 1, :]
        like = like + jnp.where(hit, logprob[r:r + 1, :], 0.0)
        cnt = cnt + jnp.where(hit, counted[r:r + 1, :], 0.0)
    eye = lax.broadcasted_iota(jnp.int32, (docs, docs), 0) == lax.broadcasted_iota(jnp.int32, (docs, docs), 1)
    for out, sums in ((like_ref, like), (cnt_ref, cnt)):
        tall = jnp.sum(sums, axis=1, keepdims=True)
        out[...] = jnp.sum(jnp.where(eye, tall, 0.0), axis=0, keepdims=True)

    def drain(c):
        c.wait_send()

    for block in [None, *range(NZ - 1)]:
        @pl.when((me_z + 1 < NZ) if block is None else (me_z > block) & (me_z + 1 < NZ))
        def _(block=block):
            for g in range(groups):
                for c in kv_copy(block, g):
                    c.wait_send()
    for i, p in enumerate(others(me_t, NY)):
        for g in range(groups):
            att_copy(g, p, i).wait_send()
        stat_copy(p, i).wait_send()
    for off in offsets:
        guarded(off, lambda z: column(z, off, drain, False))
        guarded(off, lambda z: across(z, drain, False))
        guarded(off, lambda z: diagonal(z, drain, False))
    for d in drains:
        d()


def local(
    mesh, query_vectors, key_vectors, value_vectors, out_weight, residual, post_gain, final_gain,
    vocab_weight, segment_ids, doc_starts, doc_index, targets,
):
    ND, NZ, NY = mesh.shape["dp"], mesh.shape["seq"], mesh.shape["tensor"]
    rows = query_vectors.shape[0]
    docs = doc_starts.shape[1] * ND
    blocks = ND * NZ
    fw = out_weight.shape[1]
    voc = vocab_weight
    if fw % 128 != 0:
        voc = voc.reshape(voc.shape[0], NY, fw).transpose(1, 0, 2)
    kvw, qw = key_vectors.shape[1], query_vectors.shape[1]
    heads = qw // HEAD_DIM
    groups = kvw // HEAD_DIM
    NC = 2 if ND % 2 == 0 else 1
    NX = ND // NC
    R = blocks * PAD // 128
    f32, bf16 = jnp.float32, jnp.bfloat16
    dma = pltpu.SemaphoreType.DMA
    vm = pl.BlockSpec(memory_space=pltpu.VMEM)
    anyspace = pl.BlockSpec(memory_space=pl.ANY)
    smem = pl.BlockSpec(memory_space=pltpu.SMEM)
    sums = jax.ShapeDtypeStruct((1, docs), f32)
    logprob, like, counts = pl.pallas_call(
        functools.partial(body, (ND, NZ, NY, docs)),
        out_shape=(jax.ShapeDtypeStruct((1, rows), f32), sums, sums),
        in_specs=[vm, vm, vm, anyspace, vm, vm, vm, anyspace, vm, smem, smem, vm],
        out_specs=(vm, vm, vm),
        scratch_shapes=[
            pltpu.VMEM(out_weight.shape, bf16),
            pltpu.VMEM(voc.shape, bf16),
            pltpu.VMEM((NZ, 2, rows, kvw), bf16),
            pltpu.VMEM((heads, rows, HEAD_DIM), f32),
            pltpu.VMEM((heads, rows, 128), f32),
            pltpu.VMEM((NY, rows, qw), bf16),
            pltpu.VMEM((rows, fw), f32),
            pltpu.VMEM((NY, rows, 128), f32),
            pltpu.VMEM((ND, NZ, NY, PAD, fw), bf16),
            pltpu.VMEM((ND - NC, voc.shape[-2], NZ * PAD), f32),
            pltpu.VMEM((ND, 1, NZ * PAD), jnp.int32),
            pltpu.VMEM((3 * R, 128), f32),
            pltpu.VMEM((ND, 3 * R, 128), f32),
            pltpu.VMEM((NY, 3 * R, 128), f32),
            pltpu.VMEM((NZ, 3 * R, 128), f32),
            dma((2,)),
            dma((NZ, groups, 2)), dma((NZ, groups, 2)),
            dma((NY, groups)), dma((NY, groups)),
            dma((NY,)), dma((NY,)),
            dma((ND, NZ, NY)),
            dma((NZ, 2)),
            dma((NX, NZ, NY)),
            dma((NY, NZ, NX)),
            dma((NX, NZ, NY)),
            dma((ND,)), dma((ND,)),
            dma((NY,)), dma((NY,)),
            dma((NZ,)), dma((NZ,)),
        ],
        compiler_params=pltpu.CompilerParams(
            collective_id=0, has_side_effects=True, vmem_limit_bytes=60 * 1024 * 1024
        ),
        name="packed_loglik",
    )(
        query_vectors, key_vectors, value_vectors, out_weight, residual, post_gain, final_gain, voc,
        segment_ids, doc_starts, doc_index, targets,
    )
    return (logprob, like[0], counts[0])


def solution(mesh):
    in_specs = (
        P(("dp", "seq"), "tensor"),
        P(("dp", "seq"), "tensor"),
        P(("dp", "seq"), "tensor"),
        P(None, "tensor"),
        P(("dp", "seq"), "tensor"),
        P("tensor"),
        P("tensor"),
        P(("dp", "seq", "tensor"), None),
        P("dp", "seq"),
        P("dp", None),
        P("dp", None),
        P(),
    )
    out_specs = (P("dp", "seq"), P(), P())
    return jax.shard_map(
        functools.partial(local, mesh), mesh=mesh, in_specs=in_specs, out_specs=out_specs, check_vma=False
    )
```
